32 devices in a mesh: rows: 8 (over z, y), grp: 4 (over x, core).
Axes of the slice: x: 2, y: 2, z: 4, core: 2. Of those that a mesh axis runs over, the one named last changes fastest.
Arguments:
- activations: bfloat16 [3072, 2048], P(('rows', 'grp')), may hold values from 0 to 1
- weight_tiles: bfloat16 [3, 512, 2, 128, 128], P(None, ('rows', 'grp')), may hold values from -0.75 to 0.75
- tile_index: int32 [3, 512, 1], replicated, may hold values from 0 to 511, as said below
- bias_terms: float32 [3, 65536], replicated, may hold values from -0.3 to 0.3
- demand: int32 [32, 16], P(('rows', 'grp')), may hold values from 0 to 511, as said below
Outputs:
- final_acts: bfloat16 [3072, 2048], P(('rows', 'grp'))
The draws below stay inside these ranges and needn't reach their ends.
Inputs may be any that keep to these rules, and one draw needn't show every extreme that they name: Each row of demand lists 16 distinct blocks made of whole groups [g * 4, (g + 1) * 4); every range [r * 64, (r + 1) * 64) holds either none of them or exactly one group of 4. tile_index[l, b, k] is a block of b's own group [(b // 4) * 4, (b // 4 + 1) * 4), never b itself.
All inputs are finite; a program needn't handle non-finite values.
Results may differ from the reference program's by a relative error of at most 0.0057.
Values may be sent and summed in bfloat16 or wider, within the bound.
A program may use at most 128 MiB of HBM per device.

```python
import jax
import jax.numpy as jnp
from jax import lax

NEURONS = 65536
TILE = 128
NB = 512
LAYERS = 3
K_OFF = 1
CAP = 4
BPR = 64
LIVE = 16
R_DEV = 96
TOTAL_ROWS = 3072
N_ROWS = 8
DEVICES = 32


def draw_tile_index(key, part):
    block_count = NEURONS // TILE
    offsets = jax.random.randint(jax.random.fold_in(key, 11), (LAYERS, block_count, K_OFF), 1, CAP).astype(jnp.int32)
    blocks = jnp.arange(block_count, dtype=jnp.int32)[None, :, None]
    members = (blocks % CAP + offsets) % CAP
    return (blocks // CAP * CAP + members).astype(jnp.int32)


def draw_demand(key, part):

    def one_device(dev_key):
        key_range, key_group, key_order = jax.random.split(dev_key, 3)
        ranges = jax.random.permutation(key_range, N_ROWS)[:N_ROWS // 2].astype(jnp.int32)
        groups = jax.random.randint(key_group, (N_ROWS // 2,), 0, BPR // CAP).astype(jnp.int32)
        starts = ranges * BPR + groups * CAP
        blocks = (starts[:, None] + jnp.arange(CAP, dtype=jnp.int32)[None, :]).reshape(-1)
        return jax.random.permutation(key_order, blocks).astype(jnp.int32)
    return jax.vmap(one_device)(jax.random.split(jax.random.fold_in(key, 23), DEVICES))


def shard_levels(rng, extent, shards, smallest, high):
    def one(axis_at, shards_of):
        heights = jax.random.uniform(jax.random.fold_in(jax.random.fold_in(rng, 6), axis_at), (shards_of,), jnp.float32, smallest / len(shards), high / len(shards))
        return jnp.repeat(jnp.exp(heights), extent[axis_at] // shards_of).reshape((-1,) + (1,) * (len(extent) - axis_at - 1))

    factor_of = one(*shards[0])
    for cut in shards[1:]:
        factor_of = factor_of * one(*cut)
    return factor_of


def bell_draw(rng, dims, scale, bound, shards=(), kind=jnp.bfloat16):
    gain = shard_levels(rng, dims, shards, -0.22, 0.18) if shards else 1.0
    array = jax.random.normal(rng, dims, jnp.float32) * scale * gain
    return jnp.minimum(jnp.maximum(array, -bound), bound).astype(kind)


def setup_inputs(seed: int = 0) -> dict:
    key_of = jax.random.split(jax.random.key(seed), 6)
    activations = jnp.clip(1.0 * jax.random.uniform(key_of[0], (TOTAL_ROWS, LIVE * TILE), jnp.float32) ** shard_levels(key_of[0], (TOTAL_ROWS, LIVE * TILE), ((0, 32),), -0.2, 0.2), 0.0, 1.0).astype(jnp.bfloat16)
    weight_tiles = bell_draw(key_of[1], (LAYERS, NB, 1 + K_OFF, TILE, TILE), (TILE // 2) ** -0.5, 0.75, ((1, 32),))
    tile_index = draw_tile_index(jax.random.fold_in(key_of[5], 71), 0)
    bias_terms = jnp.clip(jax.random.uniform(key_of[3], (LAYERS, NEURONS), jnp.float32, -0.3, 0.3), -0.3, 0.3)
    demand = draw_demand(jax.random.fold_in(key_of[5], 71), 0)
    return {"activations": activations, "weight_tiles": weight_tiles, "tile_index": tile_index, "bias_terms": bias_terms, "demand": demand}


def reference(activations, weight_tiles, tile_index, bias_terms, demand):
    block_count = NEURONS // TILE
    acts = activations.reshape(DEVICES, R_DEV, LIVE, TILE)
    bias_blocks = bias_terms.reshape(LAYERS, block_count, TILE)

    def one_device(inputs):
        current, live_blocks = inputs
        for layer_num in range(LAYERS):
            weights = weight_tiles[layer_num][live_blocks].astype(jnp.float32)
            off_blocks = tile_index[layer_num][live_blocks]
            matches = (off_blocks[:, :, None] == live_blocks[None, None, :]).astype(jnp.float32)
            chosen = jnp.einsum('ikp,rpt->rikt', matches, current.astype(jnp.float32))
            diag_part = jnp.einsum('rit,itu->riu', current.astype(jnp.float32), weights[:, 0])
            off_part = jnp.einsum('rikt,iktu->riu', chosen, weights[:, 1:])
            pre_act = diag_part + off_part + bias_blocks[layer_num][live_blocks][None]
            current = jax.nn.relu(pre_act).astype(jnp.bfloat16)
        return current

    result = lax.map(one_device, (acts, demand))
    return result.reshape(DEVICES * R_DEV, LIVE * TILE)
```

```python
import functools

import jax
import jax.numpy as jnp
from jax import lax
from jax.experimental import pallas as pl
from jax.experimental.pallas import tpu as pltpu
from jax.sharding import PartitionSpec as P

CAP = 4
CORES = 2
PLANES = 2
SENDS = (1, 2, 3, 6, 4, 7, 5)
MESH = pl.DeviceIdType.MESH


def group_step(state, weights, matches, bias_rows):
    chosen = jnp.einsum(
        "sckp,srpt->srckt", matches, state, preferred_element_type=jnp.float32
    ).astype(jnp.bfloat16)
    diag_part = jnp.einsum(
        "srct,sctu->srcu", state, weights[:, :, 0], preferred_element_type=jnp.float32
    )
    off_part = jnp.einsum(
        "srckt,scktu->srcu", chosen, weights[:, :, 1:], preferred_element_type=jnp.float32
    )
    return jax.nn.relu(diag_part + off_part + bias_rows[:, None]).astype(jnp.bfloat16)


def gathered_shards(activations, weight_tiles, tile_index, bias_terms, demand):
    live_blocks = demand[0]
    live_count = live_blocks.shape[0]
    tile_width = weight_tiles.shape[-1]
    row_count = lax.axis_size("rows")
    per_range = weight_tiles.shape[1] * lax.axis_size("grp")
    owners = live_blocks // per_range
    within = live_blocks % per_range
    range_ids = jnp.arange(row_count, dtype=jnp.int32)
    slot_ids = jnp.arange(CAP, dtype=jnp.int32)
    current = activations.reshape(activations.shape[0], live_count, tile_width)
    bias_blocks = bias_terms.reshape(bias_terms.shape[0], -1, tile_width)
    grouped = lax.all_gather(weight_tiles, "grp", axis=1, tiled=True)
    member = live_blocks % CAP
    placing = (owners[None, None, :] == range_ids[:, None, None]) & (
        member[None, None, :] == slot_ids[None, :, None]
    )
    starts = jnp.sum(placing[:, 0, :].astype(jnp.int32) * (within[None, :] + 1), axis=1) - 1
    outgoing = jnp.einsum(
        "acp,rpt->arct", placing.astype(jnp.bfloat16), current, preferred_element_type=jnp.float32
    ).astype(jnp.bfloat16)
    arrived = lax.all_to_all(outgoing, "rows", split_axis=0, concat_axis=0, tiled=True)
    bases = lax.all_to_all(
        starts.reshape(row_count, 1), "rows", split_axis=0, concat_axis=0, tiled=True
    )[:, 0]
    slot_blocks = jnp.clip(bases, 0)[:, None] + slot_ids[None, :]
    global_blocks = lax.axis_index("rows") * per_range + slot_blocks
    state = arrived
    for layer_num in range(weight_tiles.shape[0]):
        weights = grouped[layer_num][slot_blocks]
        off_member = tile_index[layer_num][global_blocks] % CAP
        matches = (off_member[:, :, :, None] == slot_ids[None, None, None, :]).astype(jnp.bfloat16)
        state = group_step(state, weights, matches, bias_blocks[layer_num][global_blocks])
    returned = lax.all_to_all(state, "rows", split_axis=0, concat_axis=0, tiled=True)
    current = jnp.einsum(
        "acp,arct->rpt", placing.astype(jnp.bfloat16), returned, preferred_element_type=jnp.float32
    ).astype(jnp.bfloat16)
    return current.reshape(current.shape[0], live_count * tile_width)


SCHEDULE = "F1 F2 F3 M W C0 C1 F4 C2 C3 R0 F5 R1 C4 R2 F6 R3 C5 F7 C6 R4 C7 R5 R6 R7"


def fused_kernel(
    n, demand_ref, index_ref, act_hbm, bias_hbm, w_hbm, out_ref,
    act, bias_in, bias, w_all, slots, zin, xin, ores, fres, xres, sel, fin, st_own, st_for,
    meta_out, meta_in, meta_s, in_sems, w_sems, m_send, m_recv, mx_sems, m_copy,
    z_send, z_recv, x_send, x_recv, b_send, b_recv, f_send, f_recv,
):
    layers, held = w_hbm.shape[0], w_hbm.shape[1]
    tile = w_hbm.shape[-1]
    live = demand_ref.shape[1]
    chip_blocks = held * CORES
    per_range = chip_blocks * PLANES
    r = lax.axis_index("rows")
    g = lax.axis_index("grp")
    plane, core = g // CORES, g % CORES
    mate = plane * CORES + (CORES - 1 - core)
    cross = (PLANES - 1 - plane) * CORES + core
    bits = n.bit_length() - 1

    def peer(k):
        row = 0
        for b in range(bits):
            row = row + ((r // (1 << b)) % 2 + (k >> b)) % 2 * (1 << b)
        return row

    peers = [peer(k) for k in range(n)]
    barrier = pltpu.get_barrier_semaphore()
    for k in range(n - 1, 0, -1):
        pl.semaphore_signal(barrier, inc=1, device_id=(peers[k], g), device_id_type=MESH)
    pl.semaphore_signal(barrier, inc=1, device_id=(r, cross), device_id_type=MESH)
    pl.semaphore_signal(barrier, inc=1, device_id=(r, mate), device_id_type=MESH)

    for p in range(live):
        pltpu.make_async_copy(
            act_hbm.at[:, pl.ds(p * tile, tile)], act.at[p], in_sems.at[0]
        ).start()
    act_copy = pltpu.make_async_copy(act, act, in_sems.at[0])
    first = (r * PLANES + plane) * chip_blocks
    bias_copy = pltpu.make_async_copy(
        bias_hbm.at[:, pl.ds(pl.multiple_of(first * tile, tile), chip_blocks * tile)],
        bias_in, in_sems.at[1],
    )
    bias_copy.start()
    w_local = pltpu.make_async_copy(w_hbm, w_all.at[core], w_sems.at[0])
    w_local.start()

    places = [jnp.int32(0)] * CAP
    groups = jnp.int32(0)
    for p in range(live):
        block = demand_ref[0, p]
        owner = lax.div(block, per_range)
        scale = jnp.int32(1)
        for b in range(bits):
            scale = scale * jnp.where(lax.rem(lax.div(owner, 1 << b), 2) == 1, 1 << (4 << b), 1)
        member = lax.rem(block, CAP)
        for c in range(CAP):
            places[c] = places[c] + jnp.where(member == c, p * scale, 0)
        group = lax.div(lax.rem(block, per_range), CAP)
        groups = groups + jnp.where(member == 0, group * scale, 0)
    meta_out[...] = jnp.full(meta_out.shape, groups, jnp.int32)
    meta_in[0, 0] = jnp.full(meta_out.shape, groups, jnp.int32)
    act_copy.wait()
    for k in range(n - 1, -1, -1):
        for c in range(CAP):
            pos = lax.bitwise_and(lax.shift_right_logical(places[c], peers[k] * 4), 15)
            slots[k, c] = act[pos]

    pl.semaphore_wait(barrier, n + 1)

    def meta_copy(k):
        return pltpu.make_async_remote_copy(
            src_ref=meta_out, dst_ref=meta_in.at[0, k],
            send_sem=m_send.at[k], recv_sem=m_recv.at[k],
            device_id=(peers[k], g), device_id_type=MESH,
        )

    meta_cross = pltpu.make_async_remote_copy(
        src_ref=meta_in.at[0], dst_ref=meta_in.at[1],
        send_sem=mx_sems.at[0], recv_sem=mx_sems.at[1],
        device_id=(r, cross), device_id_type=MESH,
    )

    def z_copy(k):
        return pltpu.make_async_remote_copy(
            src_ref=slots.at[k], dst_ref=zin[k],
            send_sem=z_send.at[k], recv_sem=z_recv.at[k],
            device_id=(peers[k], g), device_id_type=MESH,
        )

    def x_copy(k):
        return pltpu.make_async_remote_copy(
            src_ref=zin[k] if k else slots.at[0], dst_ref=xin[k],
            send_sem=x_send.at[k], recv_sem=x_recv.at[k],
            device_id=(r, cross), device_id_type=MESH,
        )

    def b_copy(k):
        return pltpu.make_async_remote_copy(
            src_ref=fres.at[k], dst_ref=xres.at[k],
            send_sem=b_send.at[k], recv_sem=b_recv.at[k],
            device_id=(r, cross), device_id_type=MESH,
        )

    def f_copy(k):
        return pltpu.make_async_remote_copy(
            src_ref=sel.at[k], dst_ref=fin.at[k],
            send_sem=f_send.at[k], recv_sem=f_recv.at[k],
            device_id=(peers[k], g), device_id_type=MESH,
        )

    w_remote = pltpu.make_async_remote_copy(
        src_ref=w_hbm, dst_ref=w_all.at[core],
        send_sem=w_sems.at[1], recv_sem=w_sems.at[2],
        device_id=(r, mate), device_id_type=MESH,
    )
    w_arrives = pltpu.make_async_remote_copy(
        src_ref=w_hbm, dst_ref=w_all.at[CORES - 1 - core],
        send_sem=w_sems.at[1], recv_sem=w_sems.at[2],
        device_id=(r, mate), device_id_type=MESH,
    )

    for k in SENDS:
        meta_copy(k).start()
    x_copy(0).start()
    for k in SENDS:
        z_copy(k).start()
    w_remote.start()

    def facts(which, k):
        group = lax.bitwise_and(lax.shift_right_logical(meta_s[which, k, 0, 0], r * 4), 15)
        within = group * CAP
        half = lax.rem(within, chip_blocks) // held
        return lax.div(within, chip_blocks), half, lax.rem(within, held), lax.rem(within, chip_blocks)

    def compute(k):
        near = zin[k] if k else slots.at[0]
        jobs = []
        for which, load, store, state in ((1, xin[k], fres, st_for), (0, near, ores, st_own)):
            _, half, local, inner = facts(which, k)
            jobs.append((load, store, state, half, local, inner))
        for layer in range(layers):
            for load, store, state, half, local, inner in jobs:
                for j in range(CAP):
                    other = lax.rem(index_ref[layer, 0, first + inner + j], CAP)
                    if layer == 0:
                        pair = (load[j], load[other])
                    else:
                        pair = (state[layer % 2, j], state[layer % 2, other])
                    pre = jnp.dot(
                        jnp.concatenate(pair, axis=1), w_all[half, layer, local + j],
                        preferred_element_type=jnp.float32,
                    ) + bias[inner + j][layer:layer + 1]
                    value = jnp.maximum(pre, 0.0).astype(jnp.bfloat16)
                    if layer == layers - 1:
                        store[k, j] = value
                    else:
                        state[(layer + 1) % 2, j] = value

    for token in SCHEDULE.split():
        op, k = token[0], int(token[1:] or 0)
        if op == "F":
            z_copy(k).wait_recv()
            x_copy(k).start()
        elif op == "M":
            for i in range(1, n):
                meta_copy(i).wait_recv()
            meta_cross.start()
            meta_cross.wait_recv()
            to_smem = pltpu.make_async_copy(meta_in, meta_s, m_copy)
            to_smem.start()
            to_smem.wait()
        elif op == "W":
            bias_copy.wait()
            for i in range(chip_blocks):
                bias[i] = bias_in[:, i * tile:(i + 1) * tile]
            w_local.wait()
            w_arrives.wait_recv()
        elif op == "C":
            x_copy(k).wait_recv()
            compute(k)
            b_copy(k).start()
        else:
            b_copy(k).wait_recv()
            mine = facts(0, k)[0] == plane
            for j in range(CAP):
                sel[k, j] = jnp.where(mine, ores[k, j], xres[k, j])
            if k:
                f_copy(k).start()

    for j in range(CAP):
        fin[0, j] = sel[0, j]
    for k in range(1, n):
        f_copy(k).wait_recv()
    for p in range(live):
        block = demand_ref[0, p]
        k = lax.bitwise_xor(lax.div(block, per_range), r)
        out_ref[:, p * tile:(p + 1) * tile] = fin[k, lax.rem(block, CAP)]

    for k in range(n):
        if k:
            meta_copy(k).wait_send()
            z_copy(k).wait_send()
            f_copy(k).wait_send()
        x_copy(k).wait_send()
        b_copy(k).wait_send()
    meta_cross.wait_send()
    w_remote.wait_send()


def fused_shards(activations, weight_tiles, tile_index, bias_terms, demand):
    n = lax.axis_size("rows")
    layers, held, kinds, tile, _ = weight_tiles.shape
    depth = activations.shape[0]
    chip_blocks = held * CORES
    weights = weight_tiles.reshape(layers, held, kinds * tile, tile)
    smem = pl.BlockSpec(memory_space=pltpu.SMEM)
    vmem = pl.BlockSpec(memory_space=pltpu.VMEM)
    hbm = pl.BlockSpec(memory_space=pltpu.HBM)
    slot = pltpu.VMEM((n, CAP, depth, tile), jnp.bfloat16)
    single = [pltpu.VMEM((CAP, depth, tile), jnp.bfloat16)] * n
    state = pltpu.VMEM((2, CAP, depth, tile), jnp.bfloat16)
    sems = pltpu.SemaphoreType.DMA((n,))
    return pl.pallas_call(
        functools.partial(fused_kernel, n),
        out_shape=jax.ShapeDtypeStruct(activations.shape, jnp.bfloat16),
        in_specs=[smem, smem, hbm, hbm, hbm],
        out_specs=vmem,
        scratch_shapes=[
            pltpu.VMEM((demand.shape[1], depth, tile), jnp.bfloat16),
            pltpu.VMEM((layers, chip_blocks * tile), jnp.float32),
            pltpu.VMEM((chip_blocks, layers, tile), jnp.float32),
            pltpu.VMEM((CORES, layers, held, kinds * tile, tile), jnp.bfloat16),
            slot, single, single, slot, slot, slot, slot, slot, state, state,
            pltpu.VMEM((1, 128), jnp.int32),
            pltpu.VMEM((2, n, 1, 128), jnp.int32),
            pltpu.SMEM((2, n, 1, 128), jnp.int32),
            pltpu.SemaphoreType.DMA((2,)),
            pltpu.SemaphoreType.DMA((3,)),
            sems, sems,
            pltpu.SemaphoreType.DMA((2,)),
            pltpu.SemaphoreType.DMA,
            sems, sems, sems, sems, sems, sems, sems, sems,
        ],
        compiler_params=pltpu.CompilerParams(
            collective_id=0, has_side_effects=True, vmem_limit_bytes=44 * 1024 * 1024
        ),
    )(*[
        pltpu.with_memory_space_constraint(operand, pltpu.HBM)
        for operand in (demand, tile_index.transpose(0, 2, 1), activations, bias_terms, weights)
    ])


def solution(mesh):
    rows, grp = mesh.shape["rows"], mesh.shape["grp"]

    def shards(activations, weight_tiles, tile_index, bias_terms, demand):
        held, kinds = weight_tiles.shape[1], weight_tiles.shape[2]
        fits = rows == 8 and grp == PLANES * CORES and held * grp <= 16 * CAP
        fits = fits and demand.shape[1] <= 16 and demand.shape[1] % CAP == 0
        if fits and held % CAP == 0 and kinds == 2:
            return fused_shards(activations, weight_tiles, tile_index, bias_terms, demand)
        return gathered_shards(activations, weight_tiles, tile_index, bias_terms, demand)

    return jax.shard_map(
        shards,
        mesh=mesh,
        in_specs=(
            P(("rows", "grp"), None),
            P(None, ("rows", "grp"), None, None, None),
            P(),
            P(),
            P(("rows", "grp"), None),
        ),
        out_specs=P(("rows", "grp"), None),
        check_vma=False,
    )
```

```python
import functools

import jax
import jax.numpy as jnp
from jax import lax
from jax.experimental import pallas as pl
from jax.experimental.pallas import tpu as pltpu
from jax.sharding import PartitionSpec as P

CAP = 4
CORES = 2
PLANES = 2

MESH = pl.DeviceIdType.MESH


def group_step(state, weights, matches, bias_rows):
    chosen = jnp.einsum(
        "sckp,srpt->srckt", matches, state, preferred_element_type=jnp.float32
    ).astype(jnp.bfloat16)
    diag_part = jnp.einsum(
        "srct,sctu->srcu", state, weights[:, :, 0], preferred_element_type=jnp.float32
    )
    off_part = jnp.einsum(
        "srckt,scktu->srcu", chosen, weights[:, :, 1:], preferred_element_type=jnp.float32
    )
    return jax.nn.relu(diag_part + off_part + bias_rows[:, None]).astype(jnp.bfloat16)


def gathered_shards(activations, weight_tiles, tile_index, bias_terms, demand):
    live_blocks = demand[0]
    live_count = live_blocks.shape[0]
    tile_width = weight_tiles.shape[-1]
    row_count = lax.axis_size("rows")
    per_range = weight_tiles.shape[1] * lax.axis_size("grp")
    owners = live_blocks // per_range
    within = live_blocks % per_range
    range_ids = jnp.arange(row_count, dtype=jnp.int32)
    slot_ids = jnp.arange(CAP, dtype=jnp.int32)
    current = activations.reshape(activations.shape[0], live_count, tile_width)
    bias_blocks = bias_terms.reshape(bias_terms.shape[0], -1, tile_width)
    grouped = lax.all_gather(weight_tiles, "grp", axis=1, tiled=True)
    member = live_blocks % CAP
    placing = (owners[None, None, :] == range_ids[:, None, None]) & (
        member[None, None, :] == slot_ids[None, :, None]
    )
    starts = jnp.sum(placing[:, 0, :].astype(jnp.int32) * (within[None, :] + 1), axis=1) - 1
    outgoing = jnp.einsum(
        "acp,rpt->arct", placing.astype(jnp.bfloat16), current, preferred_element_type=jnp.float32
    ).astype(jnp.bfloat16)
    arrived = lax.all_to_all(outgoing, "rows", split_axis=0, concat_axis=0, tiled=True)
    bases = lax.all_to_all(
        starts.reshape(row_count, 1), "rows", split_axis=0, concat_axis=0, tiled=True
    )[:, 0]
    slot_blocks = jnp.clip(bases, 0)[:, None] + slot_ids[None, :]
    global_blocks = lax.axis_index("rows") * per_range + slot_blocks
    state = arrived
    for layer_num in range(weight_tiles.shape[0]):
        weights = grouped[layer_num][slot_blocks]
        off_member = tile_index[layer_num][global_blocks] % CAP
        matches = (off_member[:, :, :, None] == slot_ids[None, None, None, :]).astype(jnp.bfloat16)
        state = group_step(state, weights, matches, bias_blocks[layer_num][global_blocks])
    returned = lax.all_to_all(state, "rows", split_axis=0, concat_axis=0, tiled=True)
    current = jnp.einsum(
        "acp,arct->rpt", placing.astype(jnp.bfloat16), returned, preferred_element_type=jnp.float32
    ).astype(jnp.bfloat16)
    return current.reshape(current.shape[0], live_count * tile_width)


SCHEDULE = (
    "F1", "F2", "F4", "W", "C0", "F3", "C4", "B4", "F5", "C1", "C2",
    "F6", "R4", "C3", "C5", "B5", "C6", "B2", "F7", "B6", "R5", "C7",
    "B7", "R6", "B3", "B1", "B0", "R2", "R7", "R3", "R1", "R0",
)


def fused_kernel(
    n, demand_hbm, index_hbm, act_hbm, bias_hbm, w_hbm, out_ref,
    demand_ref, index_ref, act, bias_in, bias, w_all, slots, zin, xin, ores, fres, xres, sel, fin,
    st_own, st_for, meta_s, in_sems, w_sems, tokens, m_send, m_recv, mx_send, mx_recv,
    z_send, z_recv, x_send, x_recv, b_send, b_recv, f_send, f_recv,
):
    layers, held = w_hbm.shape[0], w_hbm.shape[1]
    tile = w_hbm.shape[-1]
    live = demand_ref.shape[1]
    chip_blocks = held * CORES
    per_range = chip_blocks * PLANES
    r = lax.axis_index("rows")
    g = lax.axis_index("grp")
    plane, core = g // CORES, g % CORES
    mate = plane * CORES + (CORES - 1 - core)
    cross = (PLANES - 1 - plane) * CORES + core
    bits = n.bit_length() - 1
    inner_z = (r // 2 + 1) // 2 % 2

    def peer(k):
        row = 0
        for b in range(bits):
            row = row + ((r // (1 << b)) % 2 + (k // (1 << b)) % 2) % 2 * (1 << b)
        return row

    peers = [peer(k) for k in range(n)]
    labels = list(range(5)) + [6 - inner_z, 7 - inner_z, 5 + 2 * inner_z]

    def greet(sem):
        pl.semaphore_signal(sem, inc=1, device_id=(peers[2], g), device_id_type=MESH)

        @pl.when(inner_z == 1)
        def _():
            pl.semaphore_signal(sem, inc=1, device_id=(peers[6], g), device_id_type=MESH)

    barrier = pltpu.get_barrier_semaphore()
    greet(barrier)
    pl.semaphore_signal(barrier, inc=1, device_id=(peers[1], g), device_id_type=MESH)
    pl.semaphore_signal(barrier, inc=1, device_id=(r, cross), device_id_type=MESH)
    pl.semaphore_signal(barrier, inc=1, device_id=(r, mate), device_id_type=MESH)

    demand_copy = pltpu.make_async_copy(demand_hbm, demand_ref, in_sems.at[2])
    demand_copy.start()
    for p in range(live):
        pltpu.make_async_copy(
            act_hbm.at[:, pl.ds(p * tile, tile)], act.at[p], in_sems.at[0]
        ).start()
    act_copy = pltpu.make_async_copy(act, act, in_sems.at[0])
    index_copy = pltpu.make_async_copy(index_hbm, index_ref, in_sems.at[3])
    index_copy.start()
    first = (r * PLANES + plane) * chip_blocks
    bias_copy = pltpu.make_async_copy(
        bias_hbm.at[:, pl.ds(pl.multiple_of(first * tile, tile), chip_blocks * tile)],
        bias_in, in_sems.at[1],
    )
    bias_copy.start()
    w_local = pltpu.make_async_copy(w_hbm, w_all.at[core], w_sems.at[0])
    w_local.start()

    pl.semaphore_wait(barrier, 4 + inner_z)
    greet(tokens.at[0])
    w_remote = pltpu.make_async_remote_copy(
        src_ref=w_hbm, dst_ref=w_all.at[core],
        send_sem=w_sems.at[1], recv_sem=w_sems.at[2],
        device_id=(r, mate), device_id_type=MESH,
    )
    w_remote.start()
    demand_copy.wait()
    places = [jnp.int32(0)] * CAP
    groups = jnp.int32(0)
    for p in range(live):
        block = demand_ref[0, p]
        owner = lax.div(block, per_range)
        scale = jnp.int32(1)
        for b in range(bits):
            scale = scale * jnp.where(lax.rem(lax.div(owner, 1 << b), 2) == 1, 1 << (4 << b), 1)
        member = lax.rem(block, CAP)
        for c in range(CAP):
            places[c] = places[c] + jnp.where(member == c, p * scale, 0)
        group = lax.div(lax.rem(block, per_range), CAP)
        groups = groups + jnp.where(member == 0, group * scale, 0)
    for k in range(n):
        meta_s[0, k, 0, 0] = groups
    act_copy.wait()

    def build(k):
        for c in range(CAP):
            pos = lax.bitwise_and(lax.shift_right_logical(places[c], peers[k] * 4), 15)
            slots[k, c] = act[pos]

    def meta_copy(k):
        return pltpu.make_async_remote_copy(
            src_ref=meta_s.at[0, 0], dst_ref=meta_s.at[1, k],
            send_sem=m_send.at[k], recv_sem=m_recv.at[k],
            device_id=(peers[k], g), device_id_type=MESH,
        )

    def z_arrives(i):
        k = labels[i]
        for src, dst, sem in ((meta_s.at[0, 0], meta_s.at[1, k], m_recv), (slots.at[i], zin.at[k], z_recv)):
            pltpu.make_async_remote_copy(
                src_ref=src, dst_ref=dst, send_sem=z_send.at[i], recv_sem=sem.at[k],
                device_id=(peers[i], g), device_id_type=MESH,
            ).wait_recv()
            if sem is m_recv:
                mx_copy(i).start()

    def mx_copy(k):
        return pltpu.make_async_remote_copy(
            src_ref=meta_s.at[1 if k else 0, labels[k]], dst_ref=meta_s.at[2, k],
            send_sem=mx_send.at[k], recv_sem=mx_recv.at[k],
            device_id=(r, cross), device_id_type=MESH,
        )

    def z_copy(k):
        return pltpu.make_async_remote_copy(
            src_ref=slots.at[k], dst_ref=zin.at[k],
            send_sem=z_send.at[k], recv_sem=z_recv.at[k],
            device_id=(peers[k], g), device_id_type=MESH,
        )

    def x_copy(k):
        return pltpu.make_async_remote_copy(
            src_ref=zin.at[labels[k]] if k else slots.at[0], dst_ref=xin[k],
            send_sem=x_send.at[k], recv_sem=x_recv.at[k],
            device_id=(r, cross), device_id_type=MESH,
        )

    def b_copy(k):
        return pltpu.make_async_remote_copy(
            src_ref=fres.at[k], dst_ref=xres.at[k],
            send_sem=b_send.at[k], recv_sem=b_recv.at[k],
            device_id=(r, cross), device_id_type=MESH,
        )

    def f_copy(k):
        return pltpu.make_async_remote_copy(
            src_ref=sel.at[k], dst_ref=fin.at[labels[k]],
            send_sem=f_send.at[k], recv_sem=f_recv.at[labels[k]],
            device_id=(peer(labels[k]), g), device_id_type=MESH,
        )

    w_arrives = pltpu.make_async_remote_copy(
        src_ref=w_hbm, dst_ref=w_all.at[CORES - 1 - core],
        send_sem=w_sems.at[1], recv_sem=w_sems.at[2],
        device_id=(r, mate), device_id_type=MESH,
    )

    def send(k):
        meta_copy(k).start()
        z_copy(k).start()

    def send_if(where, k):
        @pl.when(inner_z == where)
        def _():
            send(k)

    def heard(i):
        pl.semaphore_wait(tokens.at[i], 1 + inner_z)

    build(0)
    mx_copy(0).start()
    x_copy(0).start()
    build(1)
    send(1)
    heard(0)
    greet(tokens.at[1])
    build(2)
    send(2)
    build(4)
    send(4)
    build(3)
    send(3)
    build(5)
    build(6)
    heard(1)
    greet(tokens.at[2])
    send(6)
    send(5)
    build(7)
    send_if(1, 7)
    heard(2)
    send_if(0, 7)

    def facts(which, k):
        group = lax.bitwise_and(lax.shift_right_logical(meta_s[which if k or which == 2 else 0, k if which == 2 else labels[k], 0, 0], r * 4), 15)
        within = group * CAP
        half = lax.rem(within, chip_blocks) // held
        return lax.div(within, chip_blocks), half, lax.rem(within, held), lax.rem(within, chip_blocks)

    def compute(k):
        for j in range(CAP):
            st_own[0, j] = zin[labels[k], j] if k else slots[0, j]
        jobs = []
        for which, load, store, state in ((2, xin[k], fres, st_for), (1, None, ores, st_own)):
            _, half, local, inner = facts(which, k)
            jobs.append((load, store, state, half, local, inner))
        for layer in range(layers):
            for load, store, state, half, local, inner in jobs:
                for j in range(CAP):
                    other = lax.rem(index_ref[layer, 0, first + inner + j], CAP)
                    if layer == 0 and load is not None:
                        pair = (load[j], load[other])
                    else:
                        pair = (state[layer % 2, j], state[layer % 2, other])
                    pre = jnp.dot(
                        jnp.concatenate(pair, axis=1), w_all[half, layer, local + j],
                        preferred_element_type=jnp.float32,
                    ) + bias[inner + j][layer:layer + 1]
                    value = jnp.maximum(pre, 0.0).astype(jnp.bfloat16)
                    if layer == layers - 1:
                        store[k, j] = value
                    else:
                        state[(layer + 1) % 2, j] = value

    for token in SCHEDULE:
        op, k = token[0], int(token[1:] or 0)
        if op == "F":
            z_arrives(k)
            x_copy(k).start()
        elif op == "W":
            index_copy.wait()
            bias_copy.wait()
            for i in range(chip_blocks):
                bias[i] = bias_in[:, i * tile:(i + 1) * tile]
            w_local.wait()
            w_arrives.wait_recv()
        elif op == "C":
            mx_copy(k).wait_recv()
            x_copy(k).wait_recv()
            compute(k)
        elif op == "B":
            b_copy(k).start()
        else:
            b_copy(k).wait_recv()
            mine = facts(1, k)[0] == plane
            for j in range(CAP):
                sel[k, j] = jnp.where(mine, ores[k, j], xres[k, j])
            if k:
                f_copy(k).start()

    for j in range(CAP):
        fin[0, j] = sel[0, j]
    for k in range(1, n):
        f_copy(k).wait_recv()
    for p in range(live):
        block = demand_ref[0, p]
        k = lax.bitwise_xor(lax.div(block, per_range), r)
        out_ref[:, p * tile:(p + 1) * tile] = fin[k, lax.rem(block, CAP)]

    for k in range(n):
        if k:
            meta_copy(k).wait_send()
            z_copy(k).wait_send()
            f_copy(k).wait_send()
        mx_copy(k).wait_send()
        x_copy(k).wait_send()
        b_copy(k).wait_send()
    w_remote.wait_send()


def fused_shards(activations, weight_tiles, tile_index, bias_terms, demand):
    n = lax.axis_size("rows")
    layers, held, kinds, tile, _ = weight_tiles.shape
    depth = activations.shape[0]
    chip_blocks = held * CORES
    weights = weight_tiles.reshape(layers, held, kinds * tile, tile)
    vmem = pl.BlockSpec(memory_space=pltpu.VMEM)
    hbm = pl.BlockSpec(memory_space=pltpu.HBM)
    slot = pltpu.VMEM((n, CAP, depth, tile), jnp.bfloat16)
    single = [pltpu.VMEM((CAP, depth, tile), jnp.bfloat16)] * n
    state = pltpu.VMEM((2, CAP, depth, tile), jnp.bfloat16)
    sems = pltpu.SemaphoreType.DMA((n,))
    return pl.pallas_call(
        functools.partial(fused_kernel, n),
        out_shape=jax.ShapeDtypeStruct(activations.shape, jnp.bfloat16),
        in_specs=[hbm] * 5,
        out_specs=vmem,
        scratch_shapes=[
            pltpu.SMEM(demand.shape, jnp.int32),
            pltpu.SMEM((layers, 1, tile_index.shape[1]), jnp.int32),
            pltpu.VMEM((demand.shape[1], depth, tile), jnp.bfloat16),
            pltpu.VMEM((layers, chip_blocks * tile), jnp.float32),
            pltpu.VMEM((chip_blocks, layers, tile), jnp.float32),
            pltpu.VMEM((CORES, layers, held, kinds * tile, tile), jnp.bfloat16),
            slot, slot, single, slot, slot, slot, slot, slot, state, state,
            pltpu.SMEM((3, n, 1, 128), jnp.int32),
            pltpu.SemaphoreType.DMA((4,)),
            pltpu.SemaphoreType.DMA((3,)),
            pltpu.SemaphoreType.REGULAR((3,)),
            sems, sems, sems, sems,
            sems, sems, sems, sems, sems, sems, sems, sems,
        ],
        compiler_params=pltpu.CompilerParams(
            collective_id=0, has_side_effects=True, vmem_limit_bytes=44 * 1024 * 1024
        ),
    )(*[
        pltpu.with_memory_space_constraint(operand, pltpu.HBM)
        for operand in (demand, tile_index.transpose(0, 2, 1), activations, bias_terms, weights)
    ])


def solution(mesh):
    rows, grp = mesh.shape["rows"], mesh.shape["grp"]

    def shards(activations, weight_tiles, tile_index, bias_terms, demand):
        held, kinds = weight_tiles.shape[1], weight_tiles.shape[2]
        fits = rows == 8 and grp == PLANES * CORES and held * grp <= 16 * CAP
        fits = fits and demand.shape[1] <= 16 and demand.shape[1] % CAP == 0
        if fits and held % CAP == 0 and kinds == 2:
            return fused_shards(activations, weight_tiles, tile_index, bias_terms, demand)
        return gathered_shards(activations, weight_tiles, tile_index, bias_terms, demand)

    return jax.shard_map(
        shards,
        mesh=mesh,
        in_specs=(
            P(("rows", "grp"), None),
            P(None, ("rows", "grp"), None, None, None),
            P(),
            P(),
            P(("rows", "grp"), None),
        ),
        out_specs=P(("rows", "grp"), None),
        check_vma=False,
    )
```

```python
import functools

import jax
import jax.numpy as jnp
from jax import lax
from jax.experimental import pallas as pl
from jax.experimental.pallas import tpu as pltpu
from jax.sharding import PartitionSpec as P

CAP = 4
CORES = 2
PLANES = 2
MESH = pl.DeviceIdType.MESH


def group_step(state, weights, matches, bias_rows):
    chosen = jnp.einsum(
        "sckp,srpt->srckt", matches, state, preferred_element_type=jnp.float32
    ).astype(jnp.bfloat16)
    diag_part = jnp.einsum(
        "srct,sctu->srcu", state, weights[:, :, 0], preferred_element_type=jnp.float32
    )
    off_part = jnp.einsum(
        "srckt,scktu->srcu", chosen, weights[:, :, 1:], preferred_element_type=jnp.float32
    )
    return jax.nn.relu(diag_part + off_part + bias_rows[:, None]).astype(jnp.bfloat16)


def gathered_shards(activations, weight_tiles, tile_index, bias_terms, demand):
    live_blocks = demand[0]
    live_count = live_blocks.shape[0]
    tile_width = weight_tiles.shape[-1]
    row_count = lax.axis_size("rows")
    per_range = weight_tiles.shape[1] * lax.axis_size("grp")
    owners = live_blocks // per_range
    within = live_blocks % per_range
    range_ids = jnp.arange(row_count, dtype=jnp.int32)
    slot_ids = jnp.arange(CAP, dtype=jnp.int32)
    current = activations.reshape(activations.shape[0], live_count, tile_width)
    bias_blocks = bias_terms.reshape(bias_terms.shape[0], -1, tile_width)
    grouped = lax.all_gather(weight_tiles, "grp", axis=1, tiled=True)
    member = live_blocks % CAP
    placing = (owners[None, None, :] == range_ids[:, None, None]) & (
        member[None, None, :] == slot_ids[None, :, None]
    )
    starts = jnp.sum(placing[:, 0, :].astype(jnp.int32) * (within[None, :] + 1), axis=1) - 1
    outgoing = jnp.einsum(
        "acp,rpt->arct", placing.astype(jnp.bfloat16), current, preferred_element_type=jnp.float32
    ).astype(jnp.bfloat16)
    arrived = lax.all_to_all(outgoing, "rows", split_axis=0, concat_axis=0, tiled=True)
    bases = lax.all_to_all(
        starts.reshape(row_count, 1), "rows", split_axis=0, concat_axis=0, tiled=True
    )[:, 0]
    slot_blocks = jnp.clip(bases, 0)[:, None] + slot_ids[None, :]
    global_blocks = lax.axis_index("rows") * per_range + slot_blocks
    state = arrived
    for layer_num in range(weight_tiles.shape[0]):
        weights = grouped[layer_num][slot_blocks]
        off_member = tile_index[layer_num][global_blocks] % CAP
        matches = (off_member[:, :, :, None] == slot_ids[None, None, None, :]).astype(jnp.bfloat16)
        state = group_step(state, weights, matches, bias_blocks[layer_num][global_blocks])
    returned = lax.all_to_all(state, "rows", split_axis=0, concat_axis=0, tiled=True)
    current = jnp.einsum(
        "acp,arct->rpt", placing.astype(jnp.bfloat16), returned, preferred_element_type=jnp.float32
    ).astype(jnp.bfloat16)
    return current.reshape(current.shape[0], live_count * tile_width)


SCHEDULE = (
    "F1", "F2", "F4", "W", "F3", "C0", "C4", "B4", "C1", "F5", "C2",
    "F6", "C3", "C5", "B5", "R4", "B2", "F7", "R5", "C6", "B6", "C7",
    "B3", "B7", "B1", "R6", "B0", "R7", "R3", "R1", "R2", "R0",
)


def fused_kernel(
    n, demand_hbm, index_hbm, act_hbm, bias_hbm, w_hbm, out_ref,
    demand_ref, index_ref, act, bias_in, bias, w_all, slots, zin, xin, ores, fres, xres, sel, fin,
    st_own, st_for, meta_s, in_sems, w_sems, tokens, m_send, m_recv, mx_send, mx_recv,
    z_send, z_recv, x_send, x_recv, b_send, b_recv, f_send, f_recv,
):
    layers, held = w_hbm.shape[0], w_hbm.shape[1]
    tile = w_hbm.shape[-1]
    live = demand_ref.shape[1]
    chip_blocks = held * CORES
    per_range = chip_blocks * PLANES
    r = lax.axis_index("rows")
    g = lax.axis_index("grp")
    plane, core = g // CORES, g % CORES
    mate = plane * CORES + (CORES - 1 - core)
    cross = (PLANES - 1 - plane) * CORES + core
    bits = n.bit_length() - 1
    inner_z = (r // 2 + 1) // 2 % 2

    def peer(k):
        row = 0
        for b in range(bits):
            row = row + ((r // (1 << b)) % 2 + (k // (1 << b)) % 2) % 2 * (1 << b)
        return row

    peers = [peer(k) for k in range(n)]
    labels = list(range(5)) + [6 - inner_z, 7 - inner_z, 5 + 2 * inner_z]

    def greet(sem):
        pl.semaphore_signal(sem, inc=1, device_id=(peers[2], g), device_id_type=MESH)

        @pl.when(inner_z == 1)
        def _():
            pl.semaphore_signal(sem, inc=1, device_id=(peers[6], g), device_id_type=MESH)

    barrier = pltpu.get_barrier_semaphore()
    greet(barrier)
    pl.semaphore_signal(barrier, inc=1, device_id=(peers[1], g), device_id_type=MESH)
    pl.semaphore_signal(barrier, inc=1, device_id=(r, cross), device_id_type=MESH)
    pl.semaphore_signal(barrier, inc=1, device_id=(r, mate), device_id_type=MESH)

    demand_copy = pltpu.make_async_copy(demand_hbm, demand_ref, in_sems.at[2])
    demand_copy.start()
    for p in range(live):
        pltpu.make_async_copy(
            act_hbm.at[:, pl.ds(p * tile, tile)], act.at[p], in_sems.at[0]
        ).start()
    act_copy = pltpu.make_async_copy(act, act, in_sems.at[0])
    index_copy = pltpu.make_async_copy(index_hbm, index_ref, in_sems.at[3])
    index_copy.start()
    first = (r * PLANES + plane) * chip_blocks
    bias_copy = pltpu.make_async_copy(
        bias_hbm.at[:, pl.ds(pl.multiple_of(first * tile, tile), chip_blocks * tile)],
        bias_in, in_sems.at[1],
    )
    bias_copy.start()
    w_local = pltpu.make_async_copy(w_hbm, w_all.at[core], w_sems.at[0])
    w_local.start()

    pl.semaphore_wait(barrier, 4 + inner_z)
    greet(tokens.at[0])
    w_remote = pltpu.make_async_remote_copy(
        src_ref=w_hbm, dst_ref=w_all.at[core],
        send_sem=w_sems.at[1], recv_sem=w_sems.at[2],
        device_id=(r, mate), device_id_type=MESH,
    )
    w_remote.start()
    demand_copy.wait()
    places = [jnp.int32(0)] * CAP
    groups = jnp.int32(0)
    for p in range(live):
        block = demand_ref[0, p]
        owner = lax.div(block, per_range)
        scale = jnp.int32(1)
        for b in range(bits):
            scale = scale * jnp.where(lax.rem(lax.div(owner, 1 << b), 2) == 1, 1 << (4 << b), 1)
        member = lax.rem(block, CAP)
        for c in range(CAP):
            places[c] = places[c] + jnp.where(member == c, p * scale, 0)
        group = lax.div(lax.rem(block, per_range), CAP)
        groups = groups + jnp.where(member == 0, group * scale, 0)
    for k in range(n):
        meta_s[0, k, 0, 0] = groups
    act_copy.wait()

    def build(k):
        for c in range(CAP):
            pos = lax.bitwise_and(lax.shift_right_logical(places[c], peers[k] * 4), 15)
            slots[k, c] = act[pos]

    def meta_copy(k):
        return pltpu.make_async_remote_copy(
            src_ref=meta_s.at[0, 0], dst_ref=meta_s.at[1, k],
            send_sem=m_send.at[k], recv_sem=m_recv.at[k],
            device_id=(peers[k], g), device_id_type=MESH,
        )

    def z_arrives(i):
        k = labels[i]
        for src, dst, sem in ((meta_s.at[0, 0], meta_s.at[1, k], m_recv), (slots.at[i], zin.at[k], z_recv)):
            pltpu.make_async_remote_copy(
                src_ref=src, dst_ref=dst, send_sem=z_send.at[i], recv_sem=sem.at[k],
                device_id=(peers[i], g), device_id_type=MESH,
            ).wait_recv()
            if sem is m_recv:
                mx_copy(i).start()

    def mx_copy(k):
        return pltpu.make_async_remote_copy(
            src_ref=meta_s.at[1 if k else 0, labels[k]], dst_ref=meta_s.at[2, k],
            send_sem=mx_send.at[k], recv_sem=mx_recv.at[k],
            device_id=(r, cross), device_id_type=MESH,
        )

    def z_copy(k):
        return pltpu.make_async_remote_copy(
            src_ref=slots.at[k], dst_ref=zin.at[k],
            send_sem=z_send.at[k], recv_sem=z_recv.at[k],
            device_id=(peers[k], g), device_id_type=MESH,
        )

    def x_copy(k):
        return pltpu.make_async_remote_copy(
            src_ref=zin.at[labels[k]] if k else slots.at[0], dst_ref=xin[k],
            send_sem=x_send.at[k], recv_sem=x_recv.at[k],
            device_id=(r, cross), device_id_type=MESH,
        )

    def b_copy(k):
        return pltpu.make_async_remote_copy(
            src_ref=fres.at[k], dst_ref=xres.at[k],
            send_sem=b_send.at[k], recv_sem=b_recv.at[k],
            device_id=(r, cross), device_id_type=MESH,
        )

    def f_copy(k):
        return pltpu.make_async_remote_copy(
            src_ref=sel.at[k], dst_ref=fin.at[labels[k]],
            send_sem=f_send.at[k], recv_sem=f_recv.at[labels[k]],
            device_id=(peer(labels[k]), g), device_id_type=MESH,
        )

    w_arrives = pltpu.make_async_remote_copy(
        src_ref=w_hbm, dst_ref=w_all.at[CORES - 1 - core],
        send_sem=w_sems.at[1], recv_sem=w_sems.at[2],
        device_id=(r, mate), device_id_type=MESH,
    )

    def send(k):
        meta_copy(k).start()
        z_copy(k).start()

    def send_if(where, k):
        @pl.when(inner_z == where)
        def _():
            send(k)

    def heard(i):
        pl.semaphore_wait(tokens.at[i], 1 + inner_z)

    build(0)
    mx_copy(0).start()
    x_copy(0).start()
    build(1)
    send(1)
    heard(0)
    greet(tokens.at[1])
    build(2)
    send(2)
    build(4)
    send(4)
    build(3)
    send(3)
    build(5)
    build(6)
    heard(1)
    greet(tokens.at[2])
    send(6)
    send(5)
    build(7)
    send_if(1, 7)
    heard(2)
    send_if(0, 7)

    def facts(which, k):
        group = lax.bitwise_and(lax.shift_right_logical(meta_s[which if k or which == 2 else 0, k if which == 2 else labels[k], 0, 0], r * 4), 15)
        within = group * CAP
        half = lax.rem(within, chip_blocks) // held
        return lax.div(within, chip_blocks), half, lax.rem(within, held), lax.rem(within, chip_blocks)

    def compute(k):
        for j in range(CAP):
            st_own[0, j] = zin[labels[k], j] if k else slots[0, j]
        jobs = []
        for which, load, store, state in ((2, xin[k], fres, st_for), (1, None, ores, st_own)):
            _, half, local, inner = facts(which, k)
            jobs.append((load, store, state, half, local, inner))
        for layer in range(layers):
            for load, store, state, half, local, inner in jobs:
                for j in range(CAP):
                    other = lax.rem(index_ref[layer, 0, first + inner + j], CAP)
                    if layer == 0 and load is not None:
                        pair = (load[j], load[other])
                    else:
                        pair = (state[layer % 2, j], state[layer % 2, other])
                    pre = jnp.dot(
                        jnp.concatenate(pair, axis=1), w_all[half, layer, local + j],
                        preferred_element_type=jnp.float32,
                    ) + bias[inner + j][layer:layer + 1]
                    value = jnp.maximum(pre, 0.0).astype(jnp.bfloat16)
                    if layer == layers - 1:
                        store[k, j] = value
                    else:
                        state[(layer + 1) % 2, j] = value

    for token in SCHEDULE:
        op, k = token[0], int(token[1:] or 0)
        if op == "F":
            z_arrives(k)
            x_copy(k).start()
        elif op == "W":
            index_copy.wait()
            bias_copy.wait()
            for i in range(chip_blocks):
                bias[i] = bias_in[:, i * tile:(i + 1) * tile]
            w_local.wait()
            w_arrives.wait_recv()
        elif op == "C":
            mx_copy(k).wait_recv()
            x_copy(k).wait_recv()
            compute(k)
        elif op == "B":
            b_copy(k).start()
        else:
            b_copy(k).wait_recv()
            mine = facts(1, k)[0] == plane
            for j in range(CAP):
                sel[k, j] = jnp.where(mine, ores[k, j], xres[k, j])
            if k:
                f_copy(k).start()

    for j in range(CAP):
        fin[0, j] = sel[0, j]
    for k in range(1, n):
        f_copy(k).wait_recv()
    for p in range(live):
        block = demand_ref[0, p]
        k = lax.bitwise_xor(lax.div(block, per_range), r)
        out_ref[:, p * tile:(p + 1) * tile] = fin[k, lax.rem(block, CAP)]

    for k in range(n):
        if k:
            meta_copy(k).wait_send()
            z_copy(k).wait_send()
            f_copy(k).wait_send()
        mx_copy(k).wait_send()
        x_copy(k).wait_send()
        b_copy(k).wait_send()
    w_remote.wait_send()


def fused_shards(activations, weight_tiles, tile_index, bias_terms, demand):
    n = lax.axis_size("rows")
    layers, held, kinds, tile, _ = weight_tiles.shape
    depth = activations.shape[0]
    chip_blocks = held * CORES
    weights = weight_tiles.reshape(layers, held, kinds * tile, tile)
    vmem = pl.BlockSpec(memory_space=pltpu.VMEM)
    hbm = pl.BlockSpec(memory_space=pltpu.HBM)
    slot = pltpu.VMEM((n, CAP, depth, tile), jnp.bfloat16)
    single = [pltpu.VMEM((CAP, depth, tile), jnp.bfloat16)] * n
    state = pltpu.VMEM((2, CAP, depth, tile), jnp.bfloat16)
    sems = pltpu.SemaphoreType.DMA((n,))
    return pl.pallas_call(
        functools.partial(fused_kernel, n),
        out_shape=jax.ShapeDtypeStruct(activations.shape, jnp.bfloat16),
        in_specs=[hbm] * 5,
        out_specs=vmem,
        scratch_shapes=[
            pltpu.SMEM(demand.shape, jnp.int32),
            pltpu.SMEM((layers, 1, tile_index.shape[1]), jnp.int32),
            pltpu.VMEM((demand.shape[1], depth, tile), jnp.bfloat16),
            pltpu.VMEM((layers, chip_blocks * tile), jnp.float32),
            pltpu.VMEM((chip_blocks, layers, tile), jnp.float32),
            pltpu.VMEM((CORES, layers, held, kinds * tile, tile), jnp.bfloat16),
            slot, slot, single, slot, slot, slot, slot, slot, state, state,
            pltpu.SMEM((3, n, 1, 128), jnp.int32),
            pltpu.SemaphoreType.DMA((4,)),
            pltpu.SemaphoreType.DMA((3,)),
            pltpu.SemaphoreType.REGULAR((3,)),
            sems, sems, sems, sems,
            sems, sems, sems, sems, sems, sems, sems, sems,
        ],
        compiler_params=pltpu.CompilerParams(
            collective_id=0, has_side_effects=True, vmem_limit_bytes=44 * 1024 * 1024
        ),
    )(*[
        pltpu.with_memory_space_constraint(operand, pltpu.HBM)
        for operand in (demand, tile_index.transpose(0, 2, 1), activations, bias_terms, weights)
    ])


def solution(mesh):
    rows, grp = mesh.shape["rows"], mesh.shape["grp"]

    def shards(activations, weight_tiles, tile_index, bias_terms, demand):
        held, kinds = weight_tiles.shape[1], weight_tiles.shape[2]
        fits = rows == 8 and grp == PLANES * CORES and held * grp <= 16 * CAP
        fits = fits and demand.shape[1] <= 16 and demand.shape[1] % CAP == 0
        if fits and held % CAP == 0 and kinds == 2:
            return fused_shards(activations, weight_tiles, tile_index, bias_terms, demand)
        return gathered_shards(activations, weight_tiles, tile_index, bias_terms, demand)

    return jax.shard_map(
        shards,
        mesh=mesh,
        in_specs=(
            P(("rows", "grp"), None),
            P(None, ("rows", "grp"), None, None, None),
            P(),
            P(),
            P(("rows", "grp"), None),
        ),
        out_specs=P(("rows", "grp"), None),
        check_vma=False,
    )
```

```python
import functools

import jax
import jax.numpy as jnp
from jax import lax
from jax.experimental import pallas as pl
from jax.experimental.pallas import tpu as pltpu
from jax.sharding import PartitionSpec as P

CAP = 4
CORES = 2
PLANES = 2
MESH = pl.DeviceIdType.MESH


def group_step(state, weights, matches, bias_rows):
    chosen = jnp.einsum(
        "sckp,srpt->srckt", matches, state, preferred_element_type=jnp.float32
    ).astype(jnp.bfloat16)
    diag_part = jnp.einsum(
        "srct,sctu->srcu", state, weights[:, :, 0], preferred_element_type=jnp.float32
    )
    off_part = jnp.einsum(
        "srckt,scktu->srcu", chosen, weights[:, :, 1:], preferred_element_type=jnp.float32
    )
    return jax.nn.relu(diag_part + off_part + bias_rows[:, None]).astype(jnp.bfloat16)


def gathered_shards(activations, weight_tiles, tile_index, bias_terms, demand):
    live_blocks = demand[0]
    live_count = live_blocks.shape[0]
    tile_width = weight_tiles.shape[-1]
    row_count = lax.axis_size("rows")
    per_range = weight_tiles.shape[1] * lax.axis_size("grp")
    owners = live_blocks // per_range
    within = live_blocks % per_range
    range_ids = jnp.arange(row_count, dtype=jnp.int32)
    slot_ids = jnp.arange(CAP, dtype=jnp.int32)
    current = activations.reshape(activations.shape[0], live_count, tile_width)
    bias_blocks = bias_terms.reshape(bias_terms.shape[0], -1, tile_width)
    grouped = lax.all_gather(weight_tiles, "grp", axis=1, tiled=True)
    member = live_blocks % CAP
    placing = (owners[None, None, :] == range_ids[:, None, None]) & (
        member[None, None, :] == slot_ids[None, :, None]
    )
    starts = jnp.sum(placing[:, 0, :].astype(jnp.int32) * (within[None, :] + 1), axis=1) - 1
    outgoing = jnp.einsum(
        "acp,rpt->arct", placing.astype(jnp.bfloat16), current, preferred_element_type=jnp.float32
    ).astype(jnp.bfloat16)
    arrived = lax.all_to_all(outgoing, "rows", split_axis=0, concat_axis=0, tiled=True)
    bases = lax.all_to_all(
        starts.reshape(row_count, 1), "rows", split_axis=0, concat_axis=0, tiled=True
    )[:, 0]
    slot_blocks = jnp.clip(bases, 0)[:, None] + slot_ids[None, :]
    global_blocks = lax.axis_index("rows") * per_range + slot_blocks
    state = arrived
    for layer_num in range(weight_tiles.shape[0]):
        weights = grouped[layer_num][slot_blocks]
        off_member = tile_index[layer_num][global_blocks] % CAP
        matches = (off_member[:, :, :, None] == slot_ids[None, None, None, :]).astype(jnp.bfloat16)
        state = group_step(state, weights, matches, bias_blocks[layer_num][global_blocks])
    returned = lax.all_to_all(state, "rows", split_axis=0, concat_axis=0, tiled=True)
    current = jnp.einsum(
        "acp,arct->rpt", placing.astype(jnp.bfloat16), returned, preferred_element_type=jnp.float32
    ).astype(jnp.bfloat16)
    return current.reshape(current.shape[0], live_count * tile_width)


SCHEDULE = (
    "F1", "F2", "F4", "W", "F3", "C0", "C4", "B4", "C1", "F5", "C2",
    "F6", "C3", "C5", "B5", "R4", "B2", "F7", "R5", "C6", "B6", "C7",
    "B3", "B7", "B1", "R6", "B0", "R7", "R3", "R1", "R2", "R0",
)


def fused_kernel(
    n, demand_hbm, index_hbm, act_hbm, bias_hbm, w_hbm, out_ref,
    demand_ref, index_ref, act, bias_in, bias, w_all, slots, zin, xin, ores, fres, xres, sel, fin,
    st_own, st_for, meta_s, in_sems, w_sems, tokens, m_send, m_recv, mx_send, mx_recv,
    z_send, z_recv, x_send, x_recv, b_send, b_recv, f_send, f_recv,
):
    layers, held = w_hbm.shape[0], w_hbm.shape[1]
    tile = w_hbm.shape[-1]
    live = demand_ref.shape[1]
    chip_blocks = held * CORES
    per_range = chip_blocks * PLANES
    r = lax.axis_index("rows")
    g = lax.axis_index("grp")
    plane, core = g // CORES, g % CORES
    mate = plane * CORES + (CORES - 1 - core)
    cross = (PLANES - 1 - plane) * CORES + core
    bits = n.bit_length() - 1
    inner_z = (r // 2 + 1) // 2 % 2

    def peer(k):
        row = 0
        for b in range(bits):
            row = row + ((r // (1 << b)) % 2 + (k // (1 << b)) % 2) % 2 * (1 << b)
        return row

    peers = [peer(k) for k in range(n)]
    labels = list(range(5)) + [6 - inner_z, 7 - inner_z, 5 + 2 * inner_z]

    def greet(sem):
        pl.semaphore_signal(sem, inc=1, device_id=(peers[2], g), device_id_type=MESH)

        @pl.when(inner_z == 1)
        def _():
            pl.semaphore_signal(sem, inc=1, device_id=(peers[6], g), device_id_type=MESH)

    barrier = pltpu.get_barrier_semaphore()
    greet(barrier)
    pl.semaphore_signal(barrier, inc=1, device_id=(peers[1], g), device_id_type=MESH)
    pl.semaphore_signal(barrier, inc=1, device_id=(r, cross), device_id_type=MESH)
    pl.semaphore_signal(barrier, inc=1, device_id=(r, mate), device_id_type=MESH)

    demand_copy = pltpu.make_async_copy(demand_hbm, demand_ref, in_sems.at[2])
    demand_copy.start()
    for p in range(live):
        pltpu.make_async_copy(
            act_hbm.at[:, pl.ds(p * tile, tile)], act.at[p], in_sems.at[0]
        ).start()
    act_copy = pltpu.make_async_copy(act, act, in_sems.at[0])
    index_copy = pltpu.make_async_copy(index_hbm, index_ref, in_sems.at[3])
    index_copy.start()
    first = (r * PLANES + plane) * chip_blocks
    bias_copy = pltpu.make_async_copy(
        bias_hbm.at[:, pl.ds(pl.multiple_of(first * tile, tile), chip_blocks * tile)],
        bias_in, in_sems.at[1],
    )
    bias_copy.start()
    w_local = pltpu.make_async_copy(w_hbm, w_all.at[core], w_sems.at[0])
    w_local.start()

    pl.semaphore_wait(barrier, 4 + inner_z)
    greet(tokens.at[0])
    w_remote = pltpu.make_async_remote_copy(
        src_ref=w_hbm, dst_ref=w_all.at[core],
        send_sem=w_sems.at[1], recv_sem=w_sems.at[2],
        device_id=(r, mate), device_id_type=MESH,
    )
    w_remote.start()
    demand_copy.wait()
    places = [jnp.int32(0)] * CAP
    groups = jnp.int32(0)
    for p in range(live):
        block = demand_ref[0, p]
        owner = lax.div(block, per_range)
        scale = jnp.int32(1)
        for b in range(bits):
            scale = scale * jnp.where(lax.rem(lax.div(owner, 1 << b), 2) == 1, 1 << (4 << b), 1)
        member = lax.rem(block, CAP)
        for c in range(CAP):
            places[c] = places[c] + jnp.where(member == c, p * scale, 0)
        group = lax.div(lax.rem(block, per_range), CAP)
        groups = groups + jnp.where(member == 0, group * scale, 0)
    for k in range(n):
        meta_s[0, k, 0, 0] = groups
    act_copy.wait()

    def build(k):
        for c in range(CAP):
            pos = lax.bitwise_and(lax.shift_right_logical(places[c], peers[k] * 4), 15)
            slots[k, c] = act[pos]

    def meta_copy(k):
        return pltpu.make_async_remote_copy(
            src_ref=meta_s.at[0, 0], dst_ref=meta_s.at[1, k],
            send_sem=m_send.at[k], recv_sem=m_recv.at[k],
            device_id=(peers[k], g), device_id_type=MESH,
        )

    def z_arrives(i):
        k = labels[i]
        for src, dst, sem in ((meta_s.at[0, 0], meta_s.at[1, k], m_recv), (slots.at[i], zin.at[k], z_recv)):
            pltpu.make_async_remote_copy(
                src_ref=src, dst_ref=dst, send_sem=z_send.at[i], recv_sem=sem.at[k],
                device_id=(peers[i], g), device_id_type=MESH,
            ).wait_recv()
            if sem is m_recv:
                mx_copy(i).start()

    def mx_copy(k):
        return pltpu.make_async_remote_copy(
            src_ref=meta_s.at[1 if k else 0, labels[k]], dst_ref=meta_s.at[2, k],
            send_sem=mx_send.at[k], recv_sem=mx_recv.at[k],
            device_id=(r, cross), device_id_type=MESH,
        )

    def z_copy(k):
        return pltpu.make_async_remote_copy(
            src_ref=slots.at[k], dst_ref=zin.at[k],
            send_sem=z_send.at[k], recv_sem=z_recv.at[k],
            device_id=(peers[k], g), device_id_type=MESH,
        )

    def x_copy(k):
        return pltpu.make_async_remote_copy(
            src_ref=zin.at[labels[k]] if k else slots.at[0], dst_ref=xin[k],
            send_sem=x_send.at[k], recv_sem=x_recv.at[k],
            device_id=(r, cross), device_id_type=MESH,
        )

    def b_copy(k):
        return pltpu.make_async_remote_copy(
            src_ref=fres.at[k], dst_ref=xres.at[k],
            send_sem=b_send.at[k], recv_sem=b_recv.at[k],
            device_id=(r, cross), device_id_type=MESH,
        )

    def f_copy(k):
        return pltpu.make_async_remote_copy(
            src_ref=sel.at[k], dst_ref=fin.at[labels[k]],
            send_sem=f_send.at[k], recv_sem=f_recv.at[labels[k]],
            device_id=(peer(labels[k]), g), device_id_type=MESH,
        )

    w_arrives = pltpu.make_async_remote_copy(
        src_ref=w_hbm, dst_ref=w_all.at[CORES - 1 - core],
        send_sem=w_sems.at[1], recv_sem=w_sems.at[2],
        device_id=(r, mate), device_id_type=MESH,
    )

    def send(k):
        meta_copy(k).start()
        z_copy(k).start()

    def send_if(where, k):
        @pl.when(inner_z == where)
        def _():
            send(k)

    def heard(i):
        pl.semaphore_wait(tokens.at[i], 1 + inner_z)

    build(0)
    mx_copy(0).start()
    x_copy(0).start()
    build(1)
    send(1)
    heard(0)
    greet(tokens.at[1])
    build(2)
    send(2)
    build(4)
    send(4)
    build(3)
    send(3)
    build(5)
    build(6)
    heard(1)
    greet(tokens.at[2])
    send(6)
    send(5)
    build(7)
    send_if(1, 7)
    heard(2)
    send_if(0, 7)

    def facts(which, k):
        group = lax.bitwise_and(lax.shift_right_logical(meta_s[which if k or which == 2 else 0, k if which == 2 else labels[k], 0, 0], r * 4), 15)
        within = group * CAP
        half = lax.rem(within, chip_blocks) // held
        return lax.div(within, chip_blocks), half, lax.rem(within, held), lax.rem(within, chip_blocks)

    def compute(k):
        for j in range(CAP):
            st_own[0, j] = zin[labels[k], j] if k else slots[0, j]
        jobs = []
        for which, load, store, state in ((2, xin[k], fres, st_for), (1, None, ores, st_own)):
            _, half, local, inner = facts(which, k)
            jobs.append((load, store, state, half, local, inner))
        for layer in range(layers):
            for load, store, state, half, local, inner in jobs:
                for j in range(CAP):
                    other = lax.rem(index_ref[layer, 0, first + inner + j], CAP)
                    if layer == 0 and load is not None:
                        pair = (load[j], load[other])
                    else:
                        pair = (state[layer % 2, j], state[layer % 2, other])
                    pre = jnp.dot(
                        jnp.concatenate(pair, axis=1), w_all[half, layer, local + j],
                        preferred_element_type=jnp.float32,
                    ) + bias[inner + j][layer:layer + 1]
                    value = jnp.maximum(pre, 0.0).astype(jnp.bfloat16)
                    if layer == layers - 1:
                        store[k, j] = value
                    else:
                        state[(layer + 1) % 2, j] = value

    for token in SCHEDULE:
        op, k = token[0], int(token[1:] or 0)
        if op == "F":
            z_arrives(k)
            x_copy(k).start()
        elif op == "W":
            index_copy.wait()
            bias_copy.wait()
            for i in range(chip_blocks):
                bias[i] = bias_in[:, i * tile:(i + 1) * tile]
            w_local.wait()
            w_arrives.wait_recv()
        elif op == "C":
            mx_copy(k).wait_recv()
            x_copy(k).wait_recv()
            compute(k)
        elif op == "B":
            b_copy(k).start()
        else:
            b_copy(k).wait_recv()
            mine = facts(1, k)[0] == plane
            for j in range(CAP):
                (sel if k else fin)[k, j] = jnp.where(mine, ores[k, j], xres[k, j])
            if k:
                f_copy(k).start()

    for k in range(1, n):
        f_copy(k).wait_recv()
    for p in range(live):
        block = demand_ref[0, p]
        k = lax.bitwise_xor(lax.div(block, per_range), r)
        out_ref[:, p * tile:(p + 1) * tile] = fin[k, lax.rem(block, CAP)]

    for k in range(n):
        if k:
            meta_copy(k).wait_send()
            z_copy(k).wait_send()
            f_copy(k).wait_send()
        mx_copy(k).wait_send()
        x_copy(k).wait_send()
        b_copy(k).wait_send()
    w_remote.wait_send()


def fused_shards(activations, weight_tiles, tile_index, bias_terms, demand):
    n = lax.axis_size("rows")
    layers, held, kinds, tile, _ = weight_tiles.shape
    depth = activations.shape[0]
    chip_blocks = held * CORES
    weights = weight_tiles.reshape(layers, held, kinds * tile, tile)
    vmem = pl.BlockSpec(memory_space=pltpu.VMEM)
    hbm = pl.BlockSpec(memory_space=pltpu.HBM)
    slot = pltpu.VMEM((n, CAP, depth, tile), jnp.bfloat16)
    single = [pltpu.VMEM((CAP, depth, tile), jnp.bfloat16)] * n
    state = pltpu.VMEM((2, CAP, depth, tile), jnp.bfloat16)
    sems = pltpu.SemaphoreType.DMA((n,))
    return pl.pallas_call(
        functools.partial(fused_kernel, n),
        out_shape=jax.ShapeDtypeStruct(activations.shape, jnp.bfloat16),
        in_specs=[hbm] * 5,
        out_specs=vmem,
        scratch_shapes=[
            pltpu.SMEM(demand.shape, jnp.int32),
            pltpu.SMEM((layers, 1, tile_index.shape[1]), jnp.int32),
            pltpu.VMEM((demand.shape[1], depth, tile), jnp.bfloat16),
            pltpu.VMEM((layers, chip_blocks * tile), jnp.float32),
            pltpu.VMEM((chip_blocks, layers, tile), jnp.float32),
            pltpu.VMEM((CORES, layers, held, kinds * tile, tile), jnp.bfloat16),
            slot, slot, single, slot, slot, slot, slot, slot, state, state,
            pltpu.SMEM((3, n, 1, 128), jnp.int32),
            pltpu.SemaphoreType.DMA((4,)),
            pltpu.SemaphoreType.DMA((3,)),
            pltpu.SemaphoreType.REGULAR((3,)),
            sems, sems, sems, sems,
            sems, sems, sems, sems, sems, sems, sems, sems,
        ],
        compiler_params=pltpu.CompilerParams(
            collective_id=0, has_side_effects=True, vmem_limit_bytes=44 * 1024 * 1024
        ),
    )(*[
        pltpu.with_memory_space_constraint(operand, pltpu.HBM)
        for operand in (demand, tile_index.transpose(0, 2, 1), activations, bias_terms, weights)
    ])


def solution(mesh):
    rows, grp = mesh.shape["rows"], mesh.shape["grp"]

    def shards(activations, weight_tiles, tile_index, bias_terms, demand):
        held, kinds = weight_tiles.shape[1], weight_tiles.shape[2]
        fits = rows == 8 and grp == PLANES * CORES and held * grp <= 16 * CAP
        fits = fits and demand.shape[1] <= 16 and demand.shape[1] % CAP == 0
        if fits and held % CAP == 0 and kinds == 2:
            return fused_shards(activations, weight_tiles, tile_index, bias_terms, demand)
        return gathered_shards(activations, weight_tiles, tile_index, bias_terms, demand)

    return jax.shard_map(
        shards,
        mesh=mesh,
        in_specs=(
            P(("rows", "grp"), None),
            P(None, ("rows", "grp"), None, None, None),
            P(),
            P(),
            P(("rows", "grp"), None),
        ),
        out_specs=P(("rows", "grp"), None),
        check_vma=False,
    )
```
